32 devices in a mesh: dp: 8 (over y, x, core), mp: 4 (over z).
Axes of the slice: x: 2, y: 2, z: 4, core: 2. Of those that a mesh axis runs over, the one named last changes fastest.
Arguments:
- hidden: bfloat16 [4096, 16384], P('dp', 'mp'), may hold values from -64 to 64
- key_weight: bfloat16 [16384, 1024], P(('mp', 'dp')), may hold values from -0.046875 to 0.046875
- key_state: float32 [16384], P(('mp', 'dp')), may hold values from 2.9802323e-09 to 1.1920929e-07
- key_cotangent: bfloat16 [4096, 1024], P('dp'), may hold values from -6 to 6
- doc_lengths: int32 [16, 4], P('dp'), may hold values from 1 to 128, 256 in all within a row
Outputs:
- input_grad: bfloat16 [4096, 16384], P('dp', 'mp')
- new_weight: bfloat16 [16384, 1024], P(('mp', 'dp'))
- new_state: float32 [16384], P(('mp', 'dp'))
The draws below stay inside these ranges and needn't reach their ends.
Inputs may be any that keep to these rules, and one draw needn't show every extreme that they name: `doc_lengths`: each row lists the lengths of the documents of one sequence, in order, summing to 256.
All inputs are finite; a program needn't handle non-finite values.
Results may differ from the reference program's by a relative error of at most 0.0045.
Values may be sent and summed in bfloat16 or wider, within the bound.
A program may use at most 128 MiB of HBM per device.

```python
import math
import jax
import jax.numpy as jnp
import numpy as np
from jax import lax

D = 16384
HD = 128
LEN = 256
DOCS = 4
KVW = 1024
MOST = 128
TOK_DEV = 512
SEQS = 16
TOKENS = 4096
ROWS_DEV = 512


def draw_hidden(key, part):
    draw_keys = jax.random.split(key, 5)
    base_draw = jax.random.normal(draw_keys[0], (TOKENS, D), jnp.float32)
    rising = 1.0 + 2.0 * jnp.arange(D, dtype=jnp.float32) / (D - 1)
    col_scale = jnp.exp(jax.random.uniform(draw_keys[1], (D,), jnp.float32, math.log(0.5), math.log(2.0)))
    row_scale = jnp.exp(jax.random.uniform(draw_keys[2], (TOKENS, 1), jnp.float32, math.log(0.5), math.log(2.0)))
    targets = jax.random.randint(draw_keys[4], (TOKENS // TOK_DEV,), 0, D // ROWS_DEV)
    token_block = jnp.arange(TOKENS) // TOK_DEV
    feature_block = jnp.arange(D) // ROWS_DEV
    amplified = 1.0 + 3.0 * (targets[token_block][:, None] == feature_block[None, :]).astype(jnp.float32)
    spiked = base_draw * row_scale * (col_scale * rising)[None, :] * amplified
    return jnp.clip(spiked, -64.0, 64.0).astype(jnp.bfloat16)


def level_of(stream_key, dims, shards, smallest, high):
    def one(axis_at, parts):
        steps = jax.random.uniform(jax.random.fold_in(jax.random.fold_in(stream_key, 6), axis_at), (parts,), jnp.float32, smallest / len(shards), high / len(shards))
        return jnp.repeat(jnp.exp(steps), dims[axis_at] // parts).reshape((-1,) + (1,) * (len(dims) - axis_at - 1))

    factor_of = one(*shards[0])
    for cut in shards[1:]:
        factor_of = factor_of * one(*cut)
    return factor_of


def split_up(count, total, bound, slope):
    portions = [(1 << 20) // math.isqrt(rank ** slope) + 1 for rank in range(2, count + 1)]
    rest, holding = total - bound - (count - 1), [1] * (count - 1)
    while rest > 0:
        free = [i for i in range(count - 1) if holding[i] < bound]
        pool, remaining = sum([portions[i] for i in free]), rest
        for i in free:
            addition = min(bound - holding[i], max(1, remaining * portions[i] // pool), rest)
            holding[i] = holding[i] + addition
            rest = rest - addition
    return np.array([bound] + holding)


def uneven(rng, number_of, total, bound, skew):
    if number_of == 2:
        one = jax.random.randint(rng, (), max(1, total - bound), min(bound, total - 1) + 1)
        return jnp.stack([one, total - one])
    tallies = jnp.asarray(split_up(number_of, total, bound, skew), jnp.int32)
    twos = (number_of - 1) // 2
    donor, sink = tallies[1:1 + 2 * twos:2], tallies[2:2 + 2 * twos:2]
    room = jnp.minimum(donor - 1, bound - sink)
    shifted = jax.random.randint(jax.random.fold_in(rng, 1), (twos,), 0, 1 << 20) % (room + 1)
    tallies = tallies.at[1:1 + 2 * twos:2].set(donor - shifted).at[2:2 + 2 * twos:2].set(sink + shifted)
    return tallies[jax.random.permutation(jax.random.fold_in(rng, 2), number_of)]


def normal_values(stream_key, shape, scale, reach, pieces=(), held_as=jnp.bfloat16):
    gain = level_of(stream_key, shape, pieces, -0.22, 0.18) if pieces else 1.0
    values = jax.random.normal(stream_key, shape, jnp.float32) * scale * gain
    return jnp.minimum(jnp.maximum(values, -reach), reach).astype(held_as)


def setup_inputs(seed: int = 0) -> dict:
    streams_of = jax.random.split(jax.random.key(seed), 6)
    return {
        "hidden": draw_hidden(jax.random.fold_in(streams_of[5], 71), 0),
        "key_weight": normal_values(streams_of[1], (D, KVW), D ** -0.5, 0.046875, ((0, 32),)),
        "key_state": jnp.clip(jnp.exp(math.log(1.1920928955078125e-07) - 3.6888794 * jax.random.uniform(streams_of[2], (D,), jnp.float32) ** level_of(streams_of[2], (D,), ((0, 32),), -0.2, 0.2)), 2.9802322831784522e-09, 1.1920928955078125e-07),
        "key_cotangent": normal_values(streams_of[3], (TOKENS, KVW), 1.0, 6.0, ((0, 8),)),
        "doc_lengths": jax.vmap(lambda own: uneven(own, DOCS, LEN, MOST, 1))(jax.random.split(streams_of[4], SEQS)).reshape((SEQS, DOCS)).astype(jnp.int32),
    }


learn_rate = 0.01

def positions_of(doc_lengths):
    doc_ends = jnp.cumsum(doc_lengths, axis=1).astype(jnp.int32)
    doc_starts = (doc_ends - doc_lengths).astype(jnp.int32)
    places = jnp.arange(LEN, dtype=jnp.int32)
    before = doc_starts[:, None, :] <= places[None, :, None]
    doc_start = lax.optimization_barrier(jnp.max(jnp.where(before, doc_starts[:, None, :], 0), axis=2)).astype(jnp.int32)
    return (places[None, :] - doc_start).reshape(-1).astype(jnp.int32)

def rope_back(cotangent, positions):
    half_dim = HD // 2
    frequency = jnp.exp(-(2.0 * jnp.arange(half_dim, dtype=jnp.float32) / HD) * jnp.log(jnp.float32(500000.0)))
    angles = positions.astype(jnp.float32)[:, None] * frequency[None, :]
    cos_part = jnp.cos(angles)[:, None, :]
    sin_part = jnp.sin(angles)[:, None, :]
    gradients = cotangent.astype(jnp.float32).reshape(cotangent.shape[0], -1, HD)
    first_half = gradients[..., :half_dim]
    second_half = gradients[..., half_dim:]
    rotated = jnp.concatenate([first_half * cos_part + second_half * sin_part, second_half * cos_part - first_half * sin_part], axis=-1)
    return rotated.reshape(cotangent.shape[0], -1).astype(jnp.bfloat16)

def reference(hidden, key_weight, key_state, key_cotangent, doc_lengths):
    positions = positions_of(doc_lengths)
    key_grad = rope_back(key_cotangent, positions)
    weight_grad = lax.dot_general(hidden, key_grad, (((0,), (0,)), ((), ())), preferred_element_type=jnp.float32)
    input_grad = lax.dot_general(key_grad, key_weight, (((1,), (1,)), ((), ())), preferred_element_type=jnp.float32).astype(jnp.bfloat16)
    squared = weight_grad * weight_grad
    squares_sum = jnp.sum(squared)
    clip_factor = jnp.minimum(jnp.float32(1.0), 1.0 / jnp.sqrt(squares_sum + 1e-06))
    row_mean = lax.optimization_barrier(jnp.mean(squared, axis=1))
    new_state = key_state + clip_factor * clip_factor * row_mean
    step_size = learn_rate * clip_factor * weight_grad / (jnp.sqrt(new_state)[:, None] + 1e-10)
    new_weight = (key_weight.astype(jnp.float32) - step_size).astype(jnp.bfloat16)
    return (input_grad, new_weight, new_state)
```

```python
import jax
import jax.numpy as jnp
from jax import lax
from jax.experimental import pallas as pl
from jax.experimental.pallas import tpu as pltpu
from jax.sharding import PartitionSpec as P

HD = 128
LEN = 256


learn_rate = 0.01


def positions_of(doc_lengths):
    doc_ends = jnp.cumsum(doc_lengths, axis=1)
    doc_starts = doc_ends - doc_lengths
    places = jnp.arange(LEN, dtype=jnp.int32)
    before = doc_starts[:, None, :] <= places[None, :, None]
    doc_start = jnp.max(jnp.where(before, doc_starts[:, None, :], 0), axis=2)
    return (places[None, :] - doc_start).reshape(-1)


def rope_back(cotangent, positions):
    half_dim = HD // 2
    frequency = jnp.exp(
        -(2.0 * jnp.arange(half_dim, dtype=jnp.float32) / HD) * jnp.log(jnp.float32(500000.0))
    )
    angles = positions.astype(jnp.float32)[:, None] * frequency[None, :]
    cos_part = jnp.cos(angles)[:, None, :]
    sin_part = jnp.sin(angles)[:, None, :]
    gradients = cotangent.astype(jnp.float32).reshape(cotangent.shape[0], -1, HD)
    first_half = gradients[..., :half_dim]
    second_half = gradients[..., half_dim:]
    rotated = jnp.concatenate(
        [
            first_half * cos_part + second_half * sin_part,
            second_half * cos_part - first_half * sin_part,
        ],
        axis=-1,
    )
    return rotated.reshape(cotangent.shape[0], -1).astype(jnp.bfloat16)


def update(owned, key_weight, key_state):
    squared = owned * owned
    squares_sum = lax.psum(jnp.sum(squared), ("dp", "mp"))
    clip_factor = jnp.minimum(jnp.float32(1.0), 1.0 / jnp.sqrt(squares_sum + 1e-06))
    row_mean = jnp.mean(squared, axis=1)
    new_state = key_state + clip_factor * clip_factor * row_mean
    step_size = learn_rate * clip_factor * owned / (jnp.sqrt(new_state)[:, None] + 1e-10)
    new_weight = (key_weight.astype(jnp.float32) - step_size).astype(jnp.bfloat16)
    return new_weight, new_state


def shards(hidden, key_weight, key_state, key_cotangent, doc_lengths):
    positions = positions_of(doc_lengths)
    key_grad = rope_back(key_cotangent, positions)
    gathered = lax.dot_general(
        key_grad,
        lax.all_gather(key_weight, "dp", axis=0, tiled=True),
        (((1,), (1,)), ((), ())),
        preferred_element_type=jnp.float32,
    )
    input_grad = gathered.astype(jnp.bfloat16)
    owned = lax.psum_scatter(
        lax.dot_general(
            hidden, key_grad, (((0,), (0,)), ((), ())), preferred_element_type=jnp.float32
        ),
        "dp",
        scatter_dimension=0,
        tiled=True,
    )
    return (input_grad, *update(owned, key_weight, key_state))


KG, HID, OWN_SIB, OWN_X, OWN_Y, RS1_X, RS1_Y, RS2_X, RS2_Y, FWD_X, FWD_Y, SIB_X, SIB_Y, SIB_D = (
    0, 1, 5, 6, 8, 10, 12, 14, 15, 16, 17, 18, 19, 20)
COPIES = 21


def exchange(kg, hid, w, ig, g, wall, kgs, hs, part, s1x, s1y, r1x, r1y, s2x, s2y, r2x, r2y, send, recv):
    f32 = jnp.float32
    rows = w.shape[0]
    half = rows // 2
    cols = kg.shape[1] // 2
    d = lax.axis_index("dp")
    core, xb, yb = lax.rem(d, 2), lax.rem(d // 2, 2), d // 4
    sib = d + 1 - 2 * core
    xn = d + 2 - 4 * xb
    yn = d + 4 - 8 * yb
    dg = xn + 4 - 8 * yb

    def sibling_of(block):
        return block + 1 - 2 * core

    def remote(place, src, dst, to):
        return pltpu.make_async_remote_copy(
            src_ref=src,
            dst_ref=dst,
            send_sem=send.at[place],
            recv_sem=recv.at[place],
            device_id={"dp": to},
            device_id_type=pl.DeviceIdType.MESH,
        )

    barrier = pltpu.get_barrier_semaphore()
    for to in (sib, xn, yn):
        pl.semaphore_signal(barrier, inc=1, device_id={"dp": to}, device_id_type=pl.DeviceIdType.MESH)
    pl.semaphore_wait(barrier, 3)

    def columns(block, at=0, size=None):
        size = rows if size is None else size
        return pl.ds(pl.multiple_of(block * rows + at, size), size)

    copies = {}

    def begin(place, src, dst, to):
        copies[place] = remote(place, src, dst, to)
        copies[place].start()

    first, second = pl.ds(0, half), pl.ds(half, half)
    begin(OWN_X, w.at[first], wall.at[d, first], xn)
    begin(OWN_Y, w.at[first], wall.at[d, first], yn)
    begin(KG, kg, kgs, sib)
    blocks = (dg, xn, yn, d)
    for i, block in enumerate(blocks):
        begin(HID + i, hid.at[:, columns(sibling_of(block))], hs.at[i], sib)
    begin(OWN_SIB, w, wall.at[d], sib)

    def dot_t(a, b):
        return lax.dot_general(a, b, (((0,), (0,)), ((), ())), preferred_element_type=f32)

    for i, block in enumerate(blocks):

        @pl.loop(0, 2)
        def _(t, i=i, block=block):
            part[i, pl.ds(t * half, half), :] = dot_t(hid[:, columns(block, t * half, half)], kg[...])

    copies[KG].wait_recv()
    for i, block in enumerate(blocks):
        copies[HID + i].wait_recv()

        @pl.loop(0, 2)
        def _(t, i=i):
            at = pl.ds(t * half, half)
            total = part[i, at, :] + dot_t(hs[i, :, pl.ds(pl.multiple_of(t * half, half), half)], kgs[...])
            if i == 0:
                s1x[0, at, :] = total[:, :cols].astype(jnp.bfloat16)
                s1y[0, at, :] = total[:, cols:].astype(jnp.bfloat16)
            else:
                part[i, at, :] = total
            if i == 1:
                s1x[1, at, :] = total[:, :cols].astype(jnp.bfloat16)
            if i == 2:
                s1y[1, at, :] = total[:, cols:].astype(jnp.bfloat16)

        if i == 0:
            begin(RS1_X, s1x.at[0], r1x.at[0], xn)
            begin(RS1_Y, s1y.at[0], r1y.at[0], yn)
        if i == 1:
            begin(RS1_X + 1, s1x.at[1], r1x.at[1], xn)
        if i == 2:
            begin(RS1_Y + 1, s1y.at[1], r1y.at[1], yn)
    begin(OWN_X + 1, w.at[second], wall.at[d, second], xn)
    begin(OWN_Y + 1, w.at[second], wall.at[d, second], yn)

    def multiply(weights, block):
        @pl.loop(0, 2)
        def _(t):
            ig[:, columns(block, t * half, half)] = lax.dot_general(
                kg[...], weights[pl.ds(t * half, half), :], (((1,), (1,)), ((), ())), preferred_element_type=f32
            ).astype(jnp.bfloat16)

    multiply(w, d)
    copies[OWN_SIB].wait_recv()
    multiply(wall.at[sib], sib)

    copies[RS1_X].wait_recv()

    @pl.loop(0, 2)
    def _(t):
        at = pl.ds(t * half, half)
        s2y[at, :] = (part[2, at, :cols] + r1x[0, at, :].astype(f32)).astype(jnp.bfloat16)

    begin(RS2_Y, s2y, r2y, yn)
    copies[RS1_Y].wait_recv()

    @pl.loop(0, 2)
    def _(t):
        at = pl.ds(t * half, half)
        s2x[at, :] = (part[1, at, cols:] + r1y[0, at, :].astype(f32)).astype(jnp.bfloat16)

    begin(RS2_X, s2x, r2x, xn)
    copies[OWN_X].wait_recv()
    begin(FWD_Y, wall.at[xn, first], wall.at[xn, first], yn)
    copies[OWN_Y + 1].wait_recv()
    begin(FWD_X, wall.at[yn, second], wall.at[yn, second], xn)
    copies[OWN_X + 1].wait_recv()
    begin(SIB_X, wall.at[xn], wall.at[xn], sib)
    copies[OWN_Y].wait_recv()
    begin(SIB_Y, wall.at[yn], wall.at[yn], sib)
    multiply(wall.at[xn], xn)
    multiply(wall.at[yn], yn)
    copies[SIB_X].wait_recv()
    multiply(wall.at[sibling_of(xn)], sibling_of(xn))
    copies[SIB_Y].wait_recv()
    multiply(wall.at[sibling_of(yn)], sibling_of(yn))
    copies[RS1_X + 1].wait_recv()
    copies[RS1_Y + 1].wait_recv()
    copies[RS2_X].wait_recv()
    copies[RS2_Y].wait_recv()

    @pl.loop(0, 2)
    def _(t):
        at = pl.ds(t * half, half)
        g[at, :cols] = part[3, at, :cols] + r1x[1, at, :].astype(f32) + r2y[at, :].astype(f32)
        g[at, cols:] = part[3, at, cols:] + r1y[1, at, :].astype(f32) + r2x[at, :].astype(f32)

    copies[FWD_X].wait_recv()
    copies[FWD_Y].wait_recv()
    begin(SIB_D, wall.at[dg], wall.at[dg], sib)
    multiply(wall.at[dg], dg)
    copies[SIB_D].wait_recv()
    multiply(wall.at[sibling_of(dg)], sibling_of(dg))
    for copy in copies.values():
        copy.wait_send()


def shards_cube(hidden, key_weight, key_state, key_cotangent, doc_lengths):
    key_grad = rope_back(key_cotangent, positions_of(doc_lengths))
    tokens, width = hidden.shape
    rows, kvw = key_weight.shape
    cols = kvw // 2
    bf16, f32 = jnp.bfloat16, jnp.float32
    vmem = pl.BlockSpec(memory_space=pltpu.VMEM)
    input_grad, owned = pl.pallas_call(
        exchange,
        out_shape=(
            jax.ShapeDtypeStruct((tokens, width), bf16),
            jax.ShapeDtypeStruct((rows, kvw), f32),
        ),
        in_specs=[vmem] * 3,
        out_specs=(vmem, vmem),
        scratch_shapes=[
            pltpu.VMEM((width // rows, rows, kvw), bf16),
            pltpu.VMEM((tokens, kvw), bf16),
            pltpu.VMEM((4, tokens, rows), bf16),
            pltpu.VMEM((4, rows, kvw), f32),
            pltpu.VMEM((2, rows, cols), bf16),
            pltpu.VMEM((2, rows, cols), bf16),
            pltpu.VMEM((2, rows, cols), bf16),
            pltpu.VMEM((2, rows, cols), bf16),
            pltpu.VMEM((rows, cols), bf16),
            pltpu.VMEM((rows, cols), bf16),
            pltpu.VMEM((rows, cols), bf16),
            pltpu.VMEM((rows, cols), bf16),
            pltpu.SemaphoreType.DMA((COPIES,)),
            pltpu.SemaphoreType.DMA((COPIES,)),
        ],
        compiler_params=pltpu.CompilerParams(
            collective_id=0, has_side_effects=True, vmem_limit_bytes=58 * 1024 * 1024
        ),
    )(key_grad, hidden, key_weight)
    return (input_grad, *update(owned, key_weight, key_state))


def solution(mesh):
    return jax.shard_map(
        shards_cube if mesh.shape["dp"] == 2**3 else shards,
        mesh=mesh,
        in_specs=(
            P("dp", "mp"),
            P(("mp", "dp"), None),
            P(("mp", "dp")),
            P("dp", None),
            P("dp", None),
        ),
        out_specs=(P("dp", "mp"), P(("mp", "dp"), None), P(("mp", "dp"))),
        check_vma=False,
    )
```

```python
import functools

import jax
import jax.numpy as jnp
from jax import lax
from jax.experimental import pallas as pl
from jax.experimental.pallas import tpu as pltpu
from jax.sharding import PartitionSpec as P

HD = 128
LEN = 256


learn_rate = 0.01


def positions_of(doc_lengths):
    doc_ends = jnp.cumsum(doc_lengths, axis=1)
    doc_starts = doc_ends - doc_lengths
    places = jnp.arange(LEN, dtype=jnp.int32)
    before = doc_starts[:, None, :] <= places[None, :, None]
    doc_start = jnp.max(jnp.where(before, doc_starts[:, None, :], 0), axis=2)
    return (places[None, :] - doc_start).reshape(-1)


def rope_back(cotangent, positions):
    half_dim = HD // 2
    frequency = jnp.exp(
        -(2.0 * jnp.arange(half_dim, dtype=jnp.float32) / HD) * jnp.log(jnp.float32(500000.0))
    )
    angles = positions.astype(jnp.float32)[:, None] * frequency[None, :]
    cos_part = jnp.cos(angles)[:, None, :]
    sin_part = jnp.sin(angles)[:, None, :]
    gradients = cotangent.astype(jnp.float32).reshape(cotangent.shape[0], -1, HD)
    first_half = gradients[..., :half_dim]
    second_half = gradients[..., half_dim:]
    rotated = jnp.concatenate(
        [
            first_half * cos_part + second_half * sin_part,
            second_half * cos_part - first_half * sin_part,
        ],
        axis=-1,
    )
    return rotated.reshape(cotangent.shape[0], -1).astype(jnp.bfloat16)


def update(owned, key_weight, key_state):
    squared = owned * owned
    squares_sum = lax.psum(jnp.sum(squared), ("dp", "mp"))
    clip_factor = jnp.minimum(jnp.float32(1.0), 1.0 / jnp.sqrt(squares_sum + 1e-06))
    row_mean = jnp.mean(squared, axis=1)
    new_state = key_state + clip_factor * clip_factor * row_mean
    step_size = learn_rate * clip_factor * owned / (jnp.sqrt(new_state)[:, None] + 1e-10)
    new_weight = (key_weight.astype(jnp.float32) - step_size).astype(jnp.bfloat16)
    return new_weight, new_state


def shards(hidden, key_weight, key_state, key_cotangent, doc_lengths):
    positions = positions_of(doc_lengths)
    key_grad = rope_back(key_cotangent, positions)
    gathered = lax.dot_general(
        key_grad,
        lax.all_gather(key_weight, "dp", axis=0, tiled=True),
        (((1,), (1,)), ((), ())),
        preferred_element_type=jnp.float32,
    )
    input_grad = gathered.astype(jnp.bfloat16)
    owned = lax.psum_scatter(
        lax.dot_general(
            hidden, key_grad, (((0,), (0,)), ((), ())), preferred_element_type=jnp.float32
        ),
        "dp",
        scatter_dimension=0,
        tiled=True,
    )
    return (input_grad, *update(owned, key_weight, key_state))


KG, HID, OWN_SIB, OWN_X, OWN_Y, RS1_X, RS1_Y, RS2_X, RS2_Y, FWD_X, FWD_Y, SIB_X, SIB_Y, SIB_D = (
    0, 1, 5, 6, 8, 10, 12, 14, 15, 16, 17, 18, 19, 20)
COPIES = 21


def exchange(zs, kg, hid, w, state, ig, new_w, new_state, g, squares, sums, got, wall, kgs, hs, part, s1x, s1y, r1x, r1y, s2x, s2y, r2x, r2y, send, recv, sum_send, sum_recv):
    f32 = jnp.float32
    rows = w.shape[0]
    half = rows // 2
    cols = kg.shape[1] // 2
    d = lax.axis_index("dp")
    core, xb, yb = lax.rem(d, 2), lax.rem(d // 2, 2), d // 4
    sib = d + 1 - 2 * core
    xn = d + 2 - 4 * xb
    yn = d + 4 - 8 * yb
    dg = xn + 4 - 8 * yb

    def sibling_of(block):
        return block + 1 - 2 * core

    def remote(place, src, dst, to):
        return pltpu.make_async_remote_copy(
            src_ref=src,
            dst_ref=dst,
            send_sem=send.at[place],
            recv_sem=recv.at[place],
            device_id={"dp": to},
            device_id_type=pl.DeviceIdType.MESH,
        )

    barrier = pltpu.get_barrier_semaphore()
    m = lax.axis_index("mp")
    partners = [{"mp": m + bit - 2 * bit * lax.rem(m // bit, 2)} for bit in zs]
    partners += [{"dp": sib}, {"dp": xn}, {"dp": yn}]
    for to in partners:
        pl.semaphore_signal(barrier, inc=1, device_id=to, device_id_type=pl.DeviceIdType.MESH)
    pl.semaphore_wait(barrier, len(partners))

    def columns(block, at=0, size=None):
        size = rows if size is None else size
        return pl.ds(pl.multiple_of(block * rows + at, size), size)

    copies = {}

    def begin(place, src, dst, to):
        copies[place] = remote(place, src, dst, to)
        copies[place].start()

    first, second = pl.ds(0, half), pl.ds(half, half)
    begin(OWN_X, w.at[first], wall.at[d, first], xn)
    begin(OWN_Y, w.at[first], wall.at[d, first], yn)
    begin(KG, kg, kgs, sib)
    blocks = (dg, xn, yn, d)
    for i, block in enumerate(blocks):
        begin(HID + i, hid.at[:, columns(sibling_of(block))], hs.at[i], sib)
    begin(OWN_SIB, w, wall.at[d], sib)

    def dot_t(a, b):
        return lax.dot_general(a, b, (((0,), (0,)), ((), ())), preferred_element_type=f32)

    for i, block in enumerate(blocks):

        @pl.loop(0, 2)
        def _(t, i=i, block=block):
            part[i, pl.ds(t * half, half), :] = dot_t(hid[:, columns(block, t * half, half)], kg[...])

    copies[KG].wait_recv()
    for i, block in enumerate(blocks):
        copies[HID + i].wait_recv()

        @pl.loop(0, 2)
        def _(t, i=i):
            at = pl.ds(t * half, half)
            total = part[i, at, :] + dot_t(hs[i, :, pl.ds(pl.multiple_of(t * half, half), half)], kgs[...])
            if i == 0:
                s1x[0, at, :] = total[:, :cols].astype(jnp.bfloat16)
                s1y[0, at, :] = total[:, cols:].astype(jnp.bfloat16)
            else:
                part[i, at, :] = total
            if i == 1:
                s1x[1, at, :] = total[:, :cols].astype(jnp.bfloat16)
            if i == 2:
                s1y[1, at, :] = total[:, cols:].astype(jnp.bfloat16)

        if i == 0:
            begin(RS1_X, s1x.at[0], r1x.at[0], xn)
            begin(RS1_Y, s1y.at[0], r1y.at[0], yn)
        if i == 1:
            begin(RS1_X + 1, s1x.at[1], r1x.at[1], xn)
        if i == 2:
            begin(RS1_Y + 1, s1y.at[1], r1y.at[1], yn)
    begin(OWN_X + 1, w.at[second], wall.at[d, second], xn)
    begin(OWN_Y + 1, w.at[second], wall.at[d, second], yn)

    def multiply(weights, block):
        @pl.loop(0, 2)
        def _(t):
            ig[:, columns(block, t * half, half)] = lax.dot_general(
                kg[...], weights[pl.ds(t * half, half), :], (((1,), (1,)), ((), ())), preferred_element_type=f32
            ).astype(jnp.bfloat16)

    multiply(w, d)
    copies[OWN_SIB].wait_recv()
    multiply(wall.at[sib], sib)

    copies[RS1_X].wait_recv()

    @pl.loop(0, 2)
    def _(t):
        at = pl.ds(t * half, half)
        s2y[at, :] = (part[2, at, :cols] + r1x[0, at, :].astype(f32)).astype(jnp.bfloat16)

    begin(RS2_Y, s2y, r2y, yn)
    copies[RS1_Y].wait_recv()

    @pl.loop(0, 2)
    def _(t):
        at = pl.ds(t * half, half)
        s2x[at, :] = (part[1, at, cols:] + r1y[0, at, :].astype(f32)).astype(jnp.bfloat16)

    begin(RS2_X, s2x, r2x, xn)
    copies[OWN_X].wait_recv()
    begin(FWD_Y, wall.at[xn, first], wall.at[xn, first], yn)
    copies[OWN_Y + 1].wait_recv()
    begin(FWD_X, wall.at[yn, second], wall.at[yn, second], xn)
    copies[OWN_X + 1].wait_recv()
    begin(SIB_X, wall.at[xn], wall.at[xn], sib)
    copies[OWN_Y].wait_recv()
    begin(SIB_Y, wall.at[yn], wall.at[yn], sib)
    multiply(wall.at[xn], xn)
    multiply(wall.at[yn], yn)
    copies[SIB_X].wait_recv()
    multiply(wall.at[sibling_of(xn)], sibling_of(xn))
    copies[SIB_Y].wait_recv()
    multiply(wall.at[sibling_of(yn)], sibling_of(yn))
    copies[RS1_X + 1].wait_recv()
    copies[RS1_Y + 1].wait_recv()
    copies[RS2_X].wait_recv()
    copies[RS2_Y].wait_recv()

    sums[0] = jnp.zeros_like(sums[0])

    @pl.loop(0, 8)
    def _(t):
        at = pl.ds(pl.multiple_of(t * (rows // 8), rows // 8), rows // 8)
        left = part[3, at, :cols] + r1x[1, at, :].astype(f32) + r2y[at, :].astype(f32)
        right = part[3, at, cols:] + r1y[1, at, :].astype(f32) + r2x[at, :].astype(f32)
        g[at, :cols] = left
        g[at, cols:] = right
        squared = left * left + right * right
        squares[at, :] = jnp.sum(squared, axis=1, keepdims=True)
        lanes = squared[:, :HD]
        for k in range(1, cols // HD):
            lanes += squared[:, k * HD : (k + 1) * HD]
        sums[0] += jnp.sum(lanes.reshape(rows // 64, 8, HD), axis=0)

    def sum_begin(stage):
        copy = pltpu.make_async_remote_copy(
            src_ref=sums.at[stage],
            dst_ref=got.at[stage],
            send_sem=sum_send.at[stage],
            recv_sem=sum_recv.at[stage],
            device_id=partners[stage],
            device_id_type=pl.DeviceIdType.MESH,
        )
        copies["sum", stage] = copy
        copy.start()

    def sum_end(stage):
        copies["sum", stage].wait_recv()
        sums[stage + 1] = sums[stage] + got[stage]

    last = len(partners) - 1
    for stage in range(last - 1):
        sum_begin(stage)
        sum_end(stage)
    sum_begin(last - 1)
    copies[FWD_X].wait_recv()
    copies[FWD_Y].wait_recv()
    begin(SIB_D, wall.at[dg], wall.at[dg], sib)
    sum_end(last - 1)
    sum_begin(last)
    multiply(wall.at[dg], dg)
    copies[SIB_D].wait_recv()
    multiply(wall.at[sibling_of(dg)], sibling_of(dg))
    sum_end(last)
    total = jnp.sum(jnp.sum(sums[last + 1], axis=0, keepdims=True), axis=1, keepdims=True)
    clip = jnp.minimum(1.0, 1.0 / jnp.sqrt(total + 1e-06))

    @pl.loop(0, 8)
    def _(t):
        at = pl.ds(pl.multiple_of(t * (rows // 8), rows // 8), rows // 8)
        fresh = state[at, :] + clip * clip * (squares[at, :] / w.shape[1])
        new_state[at, :] = fresh
        scale = learn_rate * clip / (jnp.sqrt(fresh) + 1e-10)
        new_w[at, :] = (w[at, :].astype(f32) - scale * g[at, :]).astype(jnp.bfloat16)

    for copy in copies.values():
        copy.wait_send()


def shards_cube(zs, hidden, key_weight, key_state, key_cotangent, doc_lengths):
    key_grad = rope_back(key_cotangent, positions_of(doc_lengths))
    tokens, width = hidden.shape
    rows, kvw = key_weight.shape
    cols = kvw // 2
    bf16, f32 = jnp.bfloat16, jnp.float32
    vmem = pl.BlockSpec(memory_space=pltpu.VMEM)
    stages = len(zs) + 3
    input_grad, new_weight, new_state = pl.pallas_call(
        functools.partial(exchange, zs),
        out_shape=(
            jax.ShapeDtypeStruct((tokens, width), bf16),
            jax.ShapeDtypeStruct((rows, kvw), bf16),
            jax.ShapeDtypeStruct((rows, 1), f32),
        ),
        in_specs=[vmem] * 4,
        out_specs=(vmem, vmem, vmem),
        scratch_shapes=[
            pltpu.VMEM((rows, kvw), f32),
            pltpu.VMEM((rows, 1), f32),
            pltpu.VMEM((stages + 1, 8, HD), f32),
            pltpu.VMEM((stages, 8, HD), f32),
            pltpu.VMEM((width // rows, rows, kvw), bf16),
            pltpu.VMEM((tokens, kvw), bf16),
            pltpu.VMEM((4, tokens, rows), bf16),
            pltpu.VMEM((4, rows, kvw), f32),
            pltpu.VMEM((2, rows, cols), bf16),
            pltpu.VMEM((2, rows, cols), bf16),
            pltpu.VMEM((2, rows, cols), bf16),
            pltpu.VMEM((2, rows, cols), bf16),
            pltpu.VMEM((rows, cols), bf16),
            pltpu.VMEM((rows, cols), bf16),
            pltpu.VMEM((rows, cols), bf16),
            pltpu.VMEM((rows, cols), bf16),
            pltpu.SemaphoreType.DMA((COPIES,)),
            pltpu.SemaphoreType.DMA((COPIES,)),
            pltpu.SemaphoreType.DMA((stages,)),
            pltpu.SemaphoreType.DMA((stages,)),
        ],
        compiler_params=pltpu.CompilerParams(
            collective_id=0, has_side_effects=True, vmem_limit_bytes=58 * 1024 * 1024
        ),
    )(key_grad, hidden, key_weight, key_state[:, None])
    return input_grad, new_weight, new_state[:, 0]


def solution(mesh):
    mp = mesh.shape["mp"]
    zs = tuple(2**k for k in range(mp.bit_length() - 1))
    cube = mesh.shape["dp"] == 2**3 and mp == 2 ** len(zs)
    return jax.shard_map(
        functools.partial(shards_cube, zs) if cube else shards,
        mesh=mesh,
        in_specs=(
            P("dp", "mp"),
            P(("mp", "dp"), None),
            P(("mp", "dp")),
            P("dp", None),
            P("dp", None),
        ),
        out_specs=(P("dp", "mp"), P(("mp", "dp"), None), P(("mp", "dp"))),
        check_vma=False,
    )
```
